32 devices in a mesh: fsdp: 8 (over z, y), tp: 4 (over x, core).
Axes of the slice: x: 2, y: 2, z: 4, core: 2. Of those that a mesh axis runs over, the one named last changes fastest.
Arguments:
- x: bfloat16 [32768, 4096], P(('fsdp', 'tp'))
- gamma: float32 [4096], replicated
- w1: bfloat16 [4096, 14336], P('fsdp', 'tp')
- w2: bfloat16 [14336, 4096], P('tp', 'fsdp')
Outputs:
- output: bfloat16 [32768, 4096], P(('fsdp', 'tp'))
All inputs are finite; a program needn't handle non-finite values.
Results may differ from the reference program's by a relative error of at most 0.001.
Values are sent between devices in bfloat16 or wider.
A program may use at most 1 GiB of HBM per device.

```python
import jax
import jax.numpy as jnp
from jax import lax

D = 4096
F = 14336
ROWS = 1024
FSDP = 8
TP = 4

TOK = FSDP * TP * ROWS
BLK = min(ROWS, 512)
EPS = 1e-6


def setup_inputs(seed: int = 0) -> dict:
    k = jax.random.split(jax.random.key(seed), 4)
    x = jax.random.normal(k[0], (TOK, D), jnp.float32).astype(jnp.bfloat16)
    gamma = jax.random.uniform(k[1], (D,), jnp.float32, 0.5, 1.5)
    w1 = (jax.random.normal(k[2], (D, F), jnp.float32) * D ** -0.5).astype(jnp.bfloat16)
    w2 = (jax.random.normal(k[3], (F, D), jnp.float32) * F ** -0.5).astype(jnp.bfloat16)
    return {"x": x, "gamma": gamma, "w1": w1, "w2": w2}


def _block(x, gamma, w1, w2):
    xf = x.astype(jnp.float32)
    mu = jnp.mean(xf, axis=-1, keepdims=True)
    var = jnp.mean(jnp.square(xf - mu), axis=-1, keepdims=True)
    xn = ((xf - mu) * lax.rsqrt(var + EPS) * gamma).astype(jnp.bfloat16)
    h = jax.nn.gelu(jnp.dot(xn, w1, preferred_element_type=jnp.float32), approximate=True).astype(jnp.bfloat16)
    y = jnp.dot(h, w2, preferred_element_type=jnp.float32)
    return (xf + y).astype(jnp.bfloat16)


def reference(x, gamma, w1, w2):
    xb = x.reshape(TOK // BLK, BLK, D)
    yb = lax.map(lambda blk: _block(blk, gamma, w1, w2), xb)
    return yb.reshape(TOK, D)
```

```python
import functools

import jax
import jax.numpy as jnp
from jax import lax
from jax.experimental import pallas as pl
from jax.experimental.pallas import tpu as pltpu
from jax.sharding import PartitionSpec as P

EPS = 1e-6
MESH = pl.DeviceIdType.MESH
BF16, F32 = jnp.bfloat16, jnp.float32

D = 4096
FS = 3584
ROWS = 1024
NC = 7
CW = FS // NC
KB = D // 8
PR = 512
HR = PR // 2


def _kernel(
    x_ref, gamma_ref, w1_ref, w2_ref,
    y_ref, xg, hg, w2g, d2d, sbuf, rs, sibp,
    w1v, xbuf, hbuf, wbuf, ubuf, dbuf, stage, tbuf, sibv, rsv, xtv, obuf,
    w1_send, w1_recv, w2_send, w2_recv, x_send, x_recv,
    dd_send, dd_recv, rs_send, rs_recv, sp_send, sp_recv,
    l_sem, loc_sem,
):
    a, b = lax.axis_index("fsdp"), lax.axis_index("tp")
    z, yq = a // 2, a % 2
    c = b % 2
    zp, zm, z2 = ((z + 1) % 4) * 2 + yq, ((z + 3) % 4) * 2 + yq, ((z + 2) % 4) * 2 + yq
    yy = z * 2 + (1 - yq)
    zpy, zmy, z2y = ((z + 1) % 4) * 2 + 1 - yq, ((z + 3) % 4) * 2 + 1 - yq, ((z + 2) % 4) * 2 + 1 - yq
    to_zp, to_zm, to_yy = (zp, b), (zm, b), (yy, b)
    sib = (a, (b // 2) * 2 + 1 - c)
    par = (a, (1 - b // 2) * 2 + c)

    barrier = pltpu.get_barrier_semaphore()
    for dev in (to_zp, to_zm, to_yy, sib, par):
        pl.semaphore_signal(barrier, inc=1, device_id=dev, device_id_type=MESH)
    pl.semaphore_wait(barrier, 5)

    def remote(src, dst, ssem, rsem, dev):
        return pltpu.make_async_remote_copy(
            src_ref=src, dst_ref=dst, send_sem=ssem, recv_sem=rsem, device_id=dev, device_id_type=MESH
        )

    sends = {}

    def w1_reg(j, s, lo, n):
        return w1v.at[j, pl.ds(pl.multiple_of(s * KB + lo, HR), n), :]

    def w1_msg(j, m, dev, s, lo=0, n=KB, own=False):
        dst = w1_reg(j, s, lo, n)
        src = w1_ref.at[:, pl.ds(j * CW, CW)] if own else dst
        cp = remote(src, dst, w1_send.at[j, m], w1_recv.at[j, m], dev)
        cp.start()
        sends[(j, m)] = cp

    def w1_got(j, m):
        sends[(j, m)].wait_recv()

    loc = {}

    def s0(j):
        w1_msg(j, 0, to_yy, a, own=True)
        w1_msg(j, 1, to_zp, a, own=True)
        w1_msg(j, 2, to_zm, a, own=True)
        cp = pltpu.make_async_copy(w1_ref.at[:, pl.ds(j * CW, CW)], w1_reg(j, a, 0, KB), loc_sem.at[j])
        cp.start()
        loc[j] = cp

    def s1(j):
        w1_got(j, 0)
        if j % 2 == 0:
            w1_msg(j, 3, to_zp, yy)
            w1_msg(j, 4, to_zm, yy)
        w1_got(j, 1)
        w1_got(j, 2)
        w1_msg(j, 5, to_zp, zm, 0, HR)
        w1_msg(j, 6, to_zm, zp, HR, HR)
        if j % 2 == 1:
            w1_msg(j, 3, to_yy, zm)
            w1_msg(j, 4, to_yy, zp)

    def s2(j):
        if j % 2 == 0:
            w1_got(j, 3)
            w1_msg(j, 7, to_zp, zmy, 0, HR)
            w1_got(j, 4)
            w1_msg(j, 8, to_zm, zpy, HR, HR)
            w1_got(j, 5)
            w1_got(j, 6)
        else:
            w1_got(j, 5)
            w1_got(j, 6)
            w1_msg(j, 7, to_yy, z2)
            w1_got(j, 3)
            w1_got(j, 4)

    def s3(j):
        w1_got(j, 7)
        if j % 2 == 0:
            w1_got(j, 8)
        loc[j].wait()

    def w2_msg(m, dev, s, lo=0, n=FS, own=False):
        dst = w2g.at[s, pl.ds(lo, n), :]
        src = w2_ref if own else dst
        return remote(src, dst, w2_send.at[m], w2_recv.at[m], dev)

    H2 = FS // 2
    w2m = [
        w2_msg(0, to_yy, a, own=True),
        w2_msg(1, to_zp, a, own=True),
        w2_msg(2, to_zm, a, own=True),
        w2_msg(3, to_zp, zm, 0, H2),
        w2_msg(4, to_zm, zp, H2, H2),
        w2_msg(5, to_yy, zm),
        w2_msg(6, to_yy, zp),
        w2_msg(7, to_yy, z2),
    ]

    s0(0)
    s0(1)
    s0(2)

    def x_in(r):
        return pltpu.make_async_copy(x_ref.at[pl.ds(r * HR, HR), :], xbuf.at[r % 2, pl.ds(0, HR), :], l_sem.at[r % 2])

    xs = {}
    x_in(0).start()
    for r in range(4):
        if r < 3:
            x_in(r + 1).start()
        x_in(r).wait()
        s = r % 2

        @pl.loop(0, HR // 32)
        def _(g):
            xf = xbuf[s, pl.ds(g * 32, 32), :].astype(F32)
            mu = jnp.mean(xf, axis=-1, keepdims=True)
            xc = xf - mu
            var = jnp.mean(jnp.square(xc), axis=-1, keepdims=True)
            xbuf[s, pl.ds(HR + g * 32, 32), :] = (xc * lax.rsqrt(var + EPS) * gamma_ref[...]).astype(BF16)

        mine = xg.at[pl.ds(r * HR, HR), :]
        cp = pltpu.make_async_copy(xbuf.at[s, pl.ds(HR, HR), :], mine, l_sem.at[2])
        cp.start()
        cp.wait()
        across = xg.at[pl.ds(pl.multiple_of(2 * ROWS + r * PR + c * HR, HR), HR), :]
        xs["p", r] = remote(mine, across, x_send.at[r], x_recv.at[r], par)
        xs["p", r].start()
        xs["s", r] = remote(mine, xg.at[pl.ds(ROWS + r * HR, HR), :], x_send.at[4 + r], x_recv.at[4 + r], sib)
        xs["s", r].start()

    def forward_x(r):
        xs["p", r].wait_recv()
        across = xg.at[pl.ds(pl.multiple_of(2 * ROWS + r * PR + c * HR, HR), HR), :]
        xs["f", r] = remote(across, across, x_send.at[8 + r], x_recv.at[8 + r], sib)
        xs["f", r].start()

    def h_tiles(n, p_of, j_of):
        def load(t, s):
            rows = pl.ds(pl.multiple_of(p_of(t) * PR, PR), PR)
            return pltpu.make_async_copy(xg.at[rows, :], xbuf.at[s], l_sem.at[s])

        def store(t, s):
            rows = pl.ds(pl.multiple_of(p_of(t) * PR, PR), PR)
            cols = pl.ds(pl.multiple_of(j_of(t) * CW, CW), CW)
            return pltpu.make_async_copy(hbuf.at[s], hg.at[rows, cols], l_sem.at[2 + s])

        load(0, 0).start()

        @pl.loop(0, n)
        def _(t):
            s = t % 2

            @pl.when(t + 1 < n)
            def _():
                load(t + 1, (t + 1) % 2).start()

            load(t, s).wait()

            @pl.when(t >= 2)
            def _():
                store(t, s).wait()

            j = j_of(t)

            @pl.loop(0, PR // HR)
            def _(r):
                rows = pl.ds(pl.multiple_of(r * HR, HR), HR)
                acc = jnp.dot(xbuf[s, rows, :], w1v[j], preferred_element_type=F32)
                hbuf[s, rows, :] = jax.nn.gelu(acc, approximate=True).astype(BF16)

            store(t, s).start()

        if n >= 2:
            store(n - 2, (n - 2) % 2).wait()
        store(n - 1, (n - 1) % 2).wait()

    def own_tiles(j):
        h_tiles(4, lambda t: t, lambda t: j)

    def got_x(r):
        xs["f", r].wait_recv()

    for t in range(NC + 2):
        if t >= 2:
            s3_ready = t - 2
        if t - 1 >= 0 and t - 1 < NC:
            s2(t - 1)
        if t < NC:
            s1(t)
            if t + 3 < NC:
                s0(t + 3)
        if t == NC - 1:
            for m in (0, 1, 2):
                w2m[m].start()
        if t in (1, 3, 5):
            forward_x(t // 2)
        if t == NC + 1:
            forward_x(3)
        if t >= 2:
            s3(s3_ready)
            if t == 2:
                for r in range(4):
                    xs["s", r].wait_recv()
            own_tiles(s3_ready)
        if t == 3:
            got_x(0)
            h_tiles(2, lambda n: 4, lambda n: n)
        if t == 4:
            h_tiles(1, lambda n: 4, lambda n: 2)
        if t == 5:
            got_x(1)
            h_tiles(5, lambda n: 4 + (n + 3) // 4, lambda n: (n + 3) % 4)
        if t == 6:
            got_x(2)
            h_tiles(5, lambda n: 4 + n // 2 - n // 4 + (n // 4) * 1, lambda n: 4) if False else h_tiles(2, lambda n: 4 + n, lambda n: 4)
            h_tiles(3, lambda n: 6, lambda n: n)
        if t == 7:
            h_tiles(2, lambda n: 4 + n, lambda n: 5)
            h_tiles(3, lambda n: 6, lambda n: 3 + n)
        if t == 8:
            got_x(3)
            h_tiles(3, lambda n: 4 + n, lambda n: 6)
            h_tiles(7, lambda n: 7, lambda n: n)

    def h_load(p, s):
        rows = pl.ds(pl.multiple_of(p * PR, PR), PR)
        return pltpu.make_async_copy(hg.at[rows, :], xbuf.at[s, :, pl.ds(0, FS)], l_sem.at[s])

    def col_of(kk):
        g = (kk + 1) // 3
        nz = (g + 1) // 2
        dz = nz * (kk % 3 + 1)
        dy = (1 - nz) * kk + g // 2
        return ((z + dz) % 4) * 2 + (yq + dy) % 2

    def dd_msg(n, s):
        return remote(ubuf.at[s, 1 - c], d2d.at[n], dd_send.at[s], dd_recv.at[n], sib)

    def rs_msg(n):
        return remote(sbuf.at[n], rs.at[n], rs_send.at[n], rs_recv.at[n], par)

    def sp_msg(n, s):
        return remote(tbuf.at[s], sibp.at[n], sp_send.at[s], sp_recv.at[n], sib)

    def pass_on(n, s):
        dd_msg(n, s).wait_recv()
        cp = pltpu.make_async_copy(d2d.at[n], dbuf, l_sem.at[2])
        cp.start()
        cp.wait()
        stage[...] = ubuf[s, c] + dbuf[...]
        cp = pltpu.make_async_copy(stage, sbuf.at[n], l_sem.at[2])
        cp.start()
        cp.wait()
        rs_msg(n).start()
        dd_msg(n, s).wait_send()

    def finish(kk, col, last):
        for p in range(2):
            h_load(p, p).start()
        cols = pl.ds(pl.multiple_of(col * KB, KB), KB)
        for p in range(2):
            h_load(p, p).wait()
            rows = pl.ds(p * PR, PR)
            n = kk * 2 + p
            sp_msg(n, p).wait_recv()
            cx = pltpu.make_async_copy(x_ref.at[rows, cols], xtv, l_sem.at[2])
            cx.start()
            cs = pltpu.make_async_copy(sibp.at[n], sibv, l_sem.at[3])
            cs.start()

            @pl.loop(0, PR // HR)
            def _(r):
                rr = pl.ds(pl.multiple_of(r * HR, HR), HR)
                tbuf[p, rr, :] = jnp.dot(xbuf[p, rr, pl.ds(0, FS)], wbuf[...], preferred_element_type=F32)

            cs.wait()
            cx.wait()

            @pl.loop(0, 2)
            def _(r):
                rr = pl.ds(pl.multiple_of(r * HR, HR), HR)
                m = kk * 4 + p * 2 + r
                rs_msg(m).wait_recv()
                cr = pltpu.make_async_copy(rs.at[m], rsv, l_sem.at[2])
                cr.start()
                cr.wait()
                total = tbuf[p, rr, :] + sibv[rr, :] + rsv[...]
                obuf[rr, :] = (xtv[rr, :].astype(F32) + total).astype(BF16)

            co = pltpu.make_async_copy(obuf, y_ref.at[rows, cols], l_sem.at[2])
            co.start()
            co.wait()

    def w2_load(kk):
        @pl.when(kk == 0)
        def _():
            cp = pltpu.make_async_copy(w2_ref, wbuf, l_sem.at[2])
            cp.start()
            cp.wait()

        @pl.when(kk > 0)
        def _():
            cp = pltpu.make_async_copy(w2g.at[col_of(kk)], wbuf, l_sem.at[2])
            cp.start()
            cp.wait()

    def own_part(kk):
        w2_load(kk)
        finish(kk, col_of(kk), False)

    @pl.loop(0, 9)
    def _(kk):
        @pl.when(kk == 1)
        def _():
            for m in (1, 2, 0):
                w2m[m].wait_recv()
            for m in (3, 4, 5, 6):
                w2m[m].start()

        @pl.when(kk == 4)
        def _():
            w2m[3].wait_recv()
            w2m[4].wait_recv()
            w2m[7].start()

        @pl.when(kk == 5)
        def _():
            w2m[5].wait_recv()

        @pl.when(kk == 6)
        def _():
            w2m[6].wait_recv()

        @pl.when(kk == 7)
        def _():
            w2m[7].wait_recv()

        @pl.when(kk < 8)
        def _():
            w2_load(kk)
            h_load(4, 0).start()

            @pl.loop(0, 4)
            def _(q):
                s = q % 2

                @pl.when(q < 3)
                def _():
                    h_load(5 + q, 1 - s).start()

                h_load(4 + q, s).wait()

                @pl.loop(0, 2)
                def _(r):
                    rr = pl.ds(pl.multiple_of(r * HR, HR), HR)
                    ubuf[s, r] = jnp.dot(xbuf[s, rr, pl.ds(0, FS)], wbuf[...], preferred_element_type=F32)

                dd_msg(kk * 4 + q, s).start()

                @pl.when(q > 0)
                def _():
                    pass_on(kk * 4 + q - 1, 1 - s)

            pass_on(kk * 4 + 3, 1)

            h_load(2, 0).start()
            h_load(3, 1).start()

            @pl.loop(0, 2)
            def _(p):
                h_load(2 + p, p).wait()

                @pl.loop(0, PR // HR)
                def _(r):
                    rr = pl.ds(pl.multiple_of(r * HR, HR), HR)
                    tbuf[p, rr, :] = jnp.dot(xbuf[p, rr, pl.ds(0, FS)], wbuf[...], preferred_element_type=F32)

                sp_msg(kk * 2 + p, p).start()

            for p in range(2):
                sp_msg(kk * 2 + p, p).wait_send()

        @pl.when(kk > 0)
        def _():
            own_part(kk - 1)

    for cp in sends.values():
        cp.wait_send()
    for cp in w2m:
        cp.wait_send()
    for cp in xs.values():
        cp.wait_send()

    @pl.loop(0, 32)
    def _(n):
        rs_msg(n).wait_send()


def _block(x, gamma, w1, w2):
    hbm = pl.BlockSpec(memory_space=pl.ANY)
    out = pl.pallas_call(
        _kernel,
        name="mlp",
        out_shape=[
            jax.ShapeDtypeStruct((ROWS, D), BF16),
            jax.ShapeDtypeStruct((4 * ROWS, D), BF16),
            jax.ShapeDtypeStruct((4 * ROWS, FS), BF16),
            jax.ShapeDtypeStruct((8, FS, KB), BF16),
            jax.ShapeDtypeStruct((32, HR, KB), F32),
            jax.ShapeDtypeStruct((32, HR, KB), F32),
            jax.ShapeDtypeStruct((32, HR, KB), F32),
            jax.ShapeDtypeStruct((16, PR, KB), F32),
        ],
        in_specs=[hbm, pl.BlockSpec(memory_space=pltpu.VMEM), hbm, hbm],
        out_specs=[hbm] * 8,
        scratch_shapes=[
            pltpu.VMEM((NC, D, CW), BF16),
            pltpu.VMEM((2, PR, D), BF16),
            pltpu.VMEM((2, PR, CW), BF16),
            pltpu.VMEM((FS, KB), BF16),
            pltpu.VMEM((2, 2, HR, KB), F32),
            pltpu.VMEM((HR, KB), F32),
            pltpu.VMEM((HR, KB), F32),
            pltpu.VMEM((2, PR, KB), F32),
            pltpu.VMEM((PR, KB), F32),
            pltpu.VMEM((HR, KB), F32),
            pltpu.VMEM((PR, KB), BF16),
            pltpu.VMEM((PR, KB), BF16),
            pltpu.SemaphoreType.DMA((NC, 9)),
            pltpu.SemaphoreType.DMA((NC, 9)),
            pltpu.SemaphoreType.DMA((8,)),
            pltpu.SemaphoreType.DMA((8,)),
            pltpu.SemaphoreType.DMA((12,)),
            pltpu.SemaphoreType.DMA((12,)),
            pltpu.SemaphoreType.DMA((2,)),
            pltpu.SemaphoreType.DMA((32,)),
            pltpu.SemaphoreType.DMA((32,)),
            pltpu.SemaphoreType.DMA((32,)),
            pltpu.SemaphoreType.DMA((2,)),
            pltpu.SemaphoreType.DMA((16,)),
            pltpu.SemaphoreType.DMA((4,)),
            pltpu.SemaphoreType.DMA((NC,)),
        ],
        compiler_params=pltpu.CompilerParams(
            collective_id=0, has_side_effects=True, vmem_limit_bytes=67000000
        ),
    )(x, gamma.reshape(1, D), w1, w2)
    return out[0]


def solution(mesh):
    return jax.shard_map(
        _block,
        mesh=mesh,
        in_specs=(P(("fsdp", "tp"), None), P(None), P("fsdp", "tp"), P("tp", "fsdp")),
        out_specs=P(("fsdp", "tp"), None),
        check_vma=False,
    )
```

```python
import functools

import jax
import jax.numpy as jnp
from jax import lax
from jax.experimental import pallas as pl
from jax.experimental.pallas import tpu as pltpu
from jax.sharding import PartitionSpec as P

EPS = 1e-6
MESH = pl.DeviceIdType.MESH
BF16, F32 = jnp.bfloat16, jnp.float32

D = 4096
FS = 3584
ROWS = 1024
NC = 7
CW = FS // NC
KB = D // 8
PR = 512
HR = PR // 2
CUT1 = KB * 27 // 32
CUT2 = FS * 27 // 32


def _kernel(
    x_ref, gamma_ref, w1_ref, w2_ref,
    y_ref, xg, hg, w2g, d2d, sbuf, rs, sibp,
    w1v, xbuf, hbuf, wbuf, ubuf, dbuf, stage, tbuf, sibv, rsv, xtv, obuf,
    w1_send, w1_recv, w2_send, w2_recv, x_send, x_recv,
    dd_send, dd_recv, rs_send, rs_recv, sp_send, sp_recv,
    l_sem, loc_sem,
):
    a, b = lax.axis_index("fsdp"), lax.axis_index("tp")
    z, yq = a // 2, a % 2
    c = b % 2
    to_zp = (lax.rem(z + 1, 4) * 2 + yq, b)
    to_zm = (lax.rem(z + 3, 4) * 2 + yq, b)
    to_yy = (z * 2 + 1 - yq, b)
    sib = (a, (b // 2) * 2 + 1 - c)
    par = (a, (1 - b // 2) * 2 + c)

    barrier = pltpu.get_barrier_semaphore()
    for dev in (to_zp, to_zm, to_yy, sib, par):
        pl.semaphore_signal(barrier, inc=1, device_id=dev, device_id_type=MESH)
    pl.semaphore_wait(barrier, 5)

    def remote(src, dst, ssem, rsem, dev):
        return pltpu.make_async_remote_copy(
            src_ref=src, dst_ref=dst, send_sem=ssem, recv_sem=rsem, device_id=dev, device_id_type=MESH
        )

    def messages(reg, own, send, recv, n, cut):
        m = {}

        def blk(dz, dy):
            return (z + dz) * 2 + (1 - yq if dy else yq)

        def add(key, dev, dz, dy, lo, cnt, sent, got, first=False):
            i = len(m)
            dst = reg(blk(dz, dy), lo, cnt)
            m[key] = (remote(own if first else dst, dst, send(i), recv(i), dev), sent, got)

        always = None
        add("Y0", to_yy, 0, 0, 0, n, always, always, True)
        for d in (1, 2, 3):
            right = (z <= 2) & (z >= d - 1)
            left = (z >= 1) & (z <= 4 - d)
            add(("R", d), to_zp, 1 - d, 0, 0, n, right, z >= d, d == 1)
            add(("L", d), to_zm, d - 1, 0, 0, n, left, z <= 3 - d, d == 1)
            add(("YL", d), to_yy, -d, 0, 0, cut, z >= d, z >= d)
            add(("YR", d), to_yy, d, 0, 0, cut, z <= 3 - d, z <= 3 - d)
            add(("BR", d), to_zp, 1 - d, 1, cut, n - cut, right, z >= d)
            add(("BL", d), to_zm, d - 1, 1, cut, n - cut, left, z <= 3 - d)
        return m

    def when(cond, f):
        if cond is None:
            f()
        else:
            pl.when(cond)(f)

    def send(m, *keys):
        for k in keys:
            when(m[k][1], m[k][0].start)

    def got(m, *keys):
        for k in keys:
            when(m[k][2], m[k][0].wait_recv)

    def stage0(m):
        send(m, "Y0", ("R", 1), ("L", 1))

    def stage1(m):
        got(m, ("R", 1), ("L", 1))
        send(m, ("R", 2), ("L", 2), ("YL", 1), ("YR", 1))
        got(m, "Y0")
        send(m, ("BR", 1), ("BL", 1))

    def stage2(m):
        got(m, ("R", 2), ("L", 2))
        send(m, ("R", 3), ("L", 3), ("YL", 2), ("YR", 2))
        got(m, ("BR", 1), ("BL", 1))
        send(m, ("BR", 2), ("BL", 2))

    def stage3(m):
        got(m, ("R", 3), ("L", 3))
        send(m, ("YL", 3), ("YR", 3))
        got(m, ("BR", 2), ("BL", 2))
        send(m, ("BR", 3), ("BL", 3))

    def stage4(m):
        for d in (1, 2, 3):
            got(m, ("YL", d), ("YR", d))
        got(m, ("BR", 3), ("BL", 3))

    def w1_messages(j):
        def reg(s, lo, n):
            return w1v.at[j, pl.ds(pl.multiple_of(s * KB + lo, 16), n), :]

        own = w1_ref.at[:, pl.ds(pl.multiple_of(j * CW, CW), CW)]
        return messages(reg, own, lambda i: w1_send.at[j, i], lambda i: w1_recv.at[j, i], KB, CUT1)

    w1m = [w1_messages(j) for j in range(NC)]
    loc = {}

    def s0(j):
        stage0(w1m[j])
        dst = w1v.at[j, pl.ds(pl.multiple_of(a * KB, KB), KB), :]
        cp = pltpu.make_async_copy(w1_ref.at[:, pl.ds(j * CW, CW)], dst, loc_sem.at[j])
        cp.start()
        loc[j] = cp

    def s1(j):
        stage1(w1m[j])

    def s2(j):
        stage2(w1m[j])

    def s3(j):
        stage3(w1m[j])

    def s4(j):
        stage4(w1m[j])
        loc[j].wait()

    w2m = messages(
        lambda s, lo, n: w2g.at[s, pl.ds(lo, n), :],
        w2_ref, lambda i: w2_send.at[i], lambda i: w2_recv.at[i], FS, CUT2,
    )

    s0(0)
    s0(1)

    def x_in(r):
        return pltpu.make_async_copy(x_ref.at[pl.ds(r * HR, HR), :], xbuf.at[r % 2, pl.ds(0, HR), :], l_sem.at[r % 2])

    xs = {}
    x_in(0).start()
    for r in range(4):
        if r < 3:
            x_in(r + 1).start()
        x_in(r).wait()
        s = r % 2

        @pl.loop(0, HR // 32)
        def _(g):
            xf = xbuf[s, pl.ds(g * 32, 32), :].astype(F32)
            mu = jnp.mean(xf, axis=-1, keepdims=True)
            xc = xf - mu
            var = jnp.mean(jnp.square(xc), axis=-1, keepdims=True)
            xbuf[s, pl.ds(HR + g * 32, 32), :] = (xc * lax.rsqrt(var + EPS) * gamma_ref[...]).astype(BF16)

        mine = xg.at[pl.ds(r * HR, HR), :]
        cp = pltpu.make_async_copy(xbuf.at[s, pl.ds(HR, HR), :], mine, l_sem.at[2])
        cp.start()
        cp.wait()
        across = xg.at[pl.ds(pl.multiple_of(2 * ROWS + r * PR + c * HR, HR), HR), :]
        xs["p", r] = remote(mine, across, x_send.at[r], x_recv.at[r], par)
        xs["p", r].start()
        xs["s", r] = remote(mine, xg.at[pl.ds(ROWS + r * HR, HR), :], x_send.at[4 + r], x_recv.at[4 + r], sib)
        xs["s", r].start()

    def forward_x(r):
        xs["p", r].wait_recv()
        across = xg.at[pl.ds(pl.multiple_of(2 * ROWS + r * PR + c * HR, HR), HR), :]
        xs["f", r] = remote(across, across, x_send.at[8 + r], x_recv.at[8 + r], sib)
        xs["f", r].start()

    def h_tiles(n, p_of, j_of):
        def load(t, s):
            rows = pl.ds(pl.multiple_of(p_of(t) * PR, PR), PR)
            return pltpu.make_async_copy(xg.at[rows, :], xbuf.at[s], l_sem.at[s])

        def store(t, s):
            rows = pl.ds(pl.multiple_of(p_of(t) * PR, PR), PR)
            cols = pl.ds(pl.multiple_of(j_of(t) * CW, CW), CW)
            return pltpu.make_async_copy(hbuf.at[s], hg.at[rows, cols], l_sem.at[2 + s])

        load(0, 0).start()

        @pl.loop(0, n)
        def _(t):
            s = t % 2

            @pl.when(t + 1 < n)
            def _():
                load(t + 1, (t + 1) % 2).start()

            load(t, s).wait()

            @pl.when(t >= 2)
            def _():
                store(t, s).wait()

            j = j_of(t)

            @pl.loop(0, PR // HR)
            def _(r):
                rows = pl.ds(pl.multiple_of(r * HR, HR), HR)
                acc = jnp.dot(xbuf[s, rows, :], w1v[j], preferred_element_type=F32)
                hbuf[s, rows, :] = jax.nn.gelu(acc, approximate=True).astype(BF16)

            store(t, s).start()

        if n >= 2:
            store(n - 2, (n - 2) % 2).wait()
        store(n - 1, (n - 1) % 2).wait()

    def own_tiles(j):
        h_tiles(4, lambda t: t, lambda t: j)

    def got_x(r):
        xs["f", r].wait_recv()

    for t in range(NC + 3):
        if 0 <= t - 2 < NC:
            s3(t - 2)
        if 0 <= t - 1 < NC:
            s2(t - 1)
        if t < NC:
            s1(t)
        if t + 2 < NC:
            s0(t + 2)
        if t == NC + 1:
            stage0(w2m)
        if 2 <= t < 6:
            forward_x(t - 2)
        if t < 3:
            continue
        j = t - 3
        s4(j)
        if t == 3:
            for r in range(4):
                xs["s", r].wait_recv()
        if j < 4:
            own_tiles(j)
            got_x(j)
            if j > 0:
                h_tiles(j, lambda n: 4 + n, lambda n: j)
            h_tiles(j + 1, lambda n: 4 + j, lambda n: n)
        else:
            h_tiles(4, lambda n: 4 + n, lambda n: j)

    def h_load(p, s):
        rows = pl.ds(pl.multiple_of(p * PR, PR), PR)
        return pltpu.make_async_copy(hg.at[rows, :], xbuf.at[s, :, pl.ds(0, FS)], l_sem.at[s])

    def pick(kk, values):
        return sum(jnp.where(kk == k, v, 0) for k, v in enumerate(values) if v)

    def col_of(kk):
        i = pick(kk, (0, 0, 1, 2, 1, 3, 2, 3))
        dy = pick(kk, (0, 1, 0, 0, 1, 0, 1, 1))
        e = jnp.where(z < 2, z, 3 - z)
        v = jnp.where(i <= e, i - 1, i)
        v = jnp.where(z < 2, v, 3 - v)
        return jnp.where(i == 0, z, v) * 2 + lax.rem(yq + dy, 2)

    def dd_msg(n, s):
        return remote(ubuf.at[s, 1 - c], d2d.at[n], dd_send.at[s], dd_recv.at[n], sib)

    def rs_msg(n):
        return remote(sbuf.at[n], rs.at[n], rs_send.at[n], rs_recv.at[n], par)

    def sp_msg(n, s):
        return remote(tbuf.at[s], sibp.at[n], sp_send.at[s], sp_recv.at[n], sib)

    def pass_on(n, s):
        dd_msg(n, s).wait_recv()
        cp = pltpu.make_async_copy(d2d.at[n], dbuf, l_sem.at[2])
        cp.start()
        cp.wait()
        stage[...] = ubuf[s, c] + dbuf[...]
        cp = pltpu.make_async_copy(stage, sbuf.at[n], l_sem.at[2])
        cp.start()
        cp.wait()
        rs_msg(n).start()
        dd_msg(n, s).wait_send()

    def finish(kk, col, last):
        for p in range(2):
            h_load(p, p).start()
        cols = pl.ds(pl.multiple_of(col * KB, KB), KB)
        for p in range(2):
            h_load(p, p).wait()
            rows = pl.ds(p * PR, PR)
            n = kk * 2 + p
            sp_msg(n, p).wait_recv()
            cx = pltpu.make_async_copy(x_ref.at[rows, cols], xtv, l_sem.at[2])
            cx.start()
            cs = pltpu.make_async_copy(sibp.at[n], sibv, l_sem.at[3])
            cs.start()

            @pl.loop(0, PR // HR)
            def _(r):
                rr = pl.ds(pl.multiple_of(r * HR, HR), HR)
                tbuf[p, rr, :] = jnp.dot(xbuf[p, rr, pl.ds(0, FS)], wbuf[...], preferred_element_type=F32)

            cs.wait()
            cx.wait()

            @pl.loop(0, 2)
            def _(r):
                rr = pl.ds(pl.multiple_of(r * HR, HR), HR)
                m = kk * 4 + p * 2 + r
                rs_msg(m).wait_recv()
                cr = pltpu.make_async_copy(rs.at[m], rsv, l_sem.at[2])
                cr.start()
                cr.wait()
                total = tbuf[p, rr, :] + sibv[rr, :] + rsv[...]
                obuf[rr, :] = (xtv[rr, :].astype(F32) + total).astype(BF16)

            co = pltpu.make_async_copy(obuf, y_ref.at[rows, cols], l_sem.at[2])
            co.start()
            co.wait()

    def w2_load(kk):
        @pl.when(kk == 0)
        def _():
            cp = pltpu.make_async_copy(w2_ref, wbuf, l_sem.at[2])
            cp.start()
            cp.wait()

        @pl.when(kk > 0)
        def _():
            cp = pltpu.make_async_copy(w2g.at[col_of(kk)], wbuf, l_sem.at[2])
            cp.start()
            cp.wait()

    def own_part(kk):
        w2_load(kk)
        finish(kk, col_of(kk), False)

    @pl.loop(0, 9)
    def _(kk):
        @pl.when(kk == 1)
        def _():
            stage1(w2m)

        @pl.when(kk == 3)
        def _():
            stage2(w2m)
            got(w2m, ("YL", 1), ("YR", 1))

        @pl.when(kk == 5)
        def _():
            stage3(w2m)
            got(w2m, ("YL", 2), ("YR", 2))

        @pl.when(kk == 6)
        def _():
            got(w2m, ("BR", 3), ("BL", 3))

        @pl.when(kk == 7)
        def _():
            got(w2m, ("YL", 3), ("YR", 3))

        @pl.when(kk < 8)
        def _():
            w2_load(kk)
            h_load(4, 0).start()

            @pl.loop(0, 4)
            def _(q):
                s = q % 2

                @pl.when(q < 3)
                def _():
                    h_load(5 + q, 1 - s).start()

                h_load(4 + q, s).wait()

                @pl.loop(0, 2)
                def _(r):
                    rr = pl.ds(pl.multiple_of(r * HR, HR), HR)
                    ubuf[s, r] = jnp.dot(xbuf[s, rr, pl.ds(0, FS)], wbuf[...], preferred_element_type=F32)

                dd_msg(kk * 4 + q, s).start()

                @pl.when(q > 0)
                def _():
                    pass_on(kk * 4 + q - 1, 1 - s)

            pass_on(kk * 4 + 3, 1)

            @pl.when(kk == 0)
            def _():
                h_tiles(12, lambda n: n % 4, lambda n: 4 + n // 4)

            h_load(2, 0).start()
            h_load(3, 1).start()

            @pl.loop(0, 2)
            def _(p):
                h_load(2 + p, p).wait()

                @pl.loop(0, PR // HR)
                def _(r):
                    rr = pl.ds(pl.multiple_of(r * HR, HR), HR)
                    tbuf[p, rr, :] = jnp.dot(xbuf[p, rr, pl.ds(0, FS)], wbuf[...], preferred_element_type=F32)

                sp_msg(kk * 2 + p, p).start()

            for p in range(2):
                sp_msg(kk * 2 + p, p).wait_send()

        @pl.when(kk > 0)
        def _():
            own_part(kk - 1)

    for m in (*w1m, w2m):
        for cp, sent, _ in m.values():
            when(sent, cp.wait_send)
    for cp in xs.values():
        cp.wait_send()

    @pl.loop(0, 32)
    def _(n):
        rs_msg(n).wait_send()


def _block(x, gamma, w1, w2):
    hbm = pl.BlockSpec(memory_space=pl.ANY)
    out = pl.pallas_call(
        _kernel,
        name="mlp",
        out_shape=[
            jax.ShapeDtypeStruct((ROWS, D), BF16),
            jax.ShapeDtypeStruct((4 * ROWS, D), BF16),
            jax.ShapeDtypeStruct((4 * ROWS, FS), BF16),
            jax.ShapeDtypeStruct((8, FS, KB), BF16),
            jax.ShapeDtypeStruct((32, HR, KB), F32),
            jax.ShapeDtypeStruct((32, HR, KB), F32),
            jax.ShapeDtypeStruct((32, HR, KB), F32),
            jax.ShapeDtypeStruct((16, PR, KB), F32),
        ],
        in_specs=[hbm, pl.BlockSpec(memory_space=pltpu.VMEM), hbm, hbm],
        out_specs=[hbm] * 8,
        scratch_shapes=[
            pltpu.VMEM((NC, D, CW), BF16),
            pltpu.VMEM((2, PR, D), BF16),
            pltpu.VMEM((2, PR, CW), BF16),
            pltpu.VMEM((FS, KB), BF16),
            pltpu.VMEM((2, 2, HR, KB), F32),
            pltpu.VMEM((HR, KB), F32),
            pltpu.VMEM((HR, KB), F32),
            pltpu.VMEM((2, PR, KB), F32),
            pltpu.VMEM((PR, KB), F32),
            pltpu.VMEM((HR, KB), F32),
            pltpu.VMEM((PR, KB), BF16),
            pltpu.VMEM((PR, KB), BF16),
            pltpu.SemaphoreType.DMA((NC, 19)),
            pltpu.SemaphoreType.DMA((NC, 19)),
            pltpu.SemaphoreType.DMA((19,)),
            pltpu.SemaphoreType.DMA((19,)),
            pltpu.SemaphoreType.DMA((12,)),
            pltpu.SemaphoreType.DMA((12,)),
            pltpu.SemaphoreType.DMA((2,)),
            pltpu.SemaphoreType.DMA((32,)),
            pltpu.SemaphoreType.DMA((32,)),
            pltpu.SemaphoreType.DMA((32,)),
            pltpu.SemaphoreType.DMA((2,)),
            pltpu.SemaphoreType.DMA((16,)),
            pltpu.SemaphoreType.DMA((4,)),
            pltpu.SemaphoreType.DMA((NC,)),
        ],
        compiler_params=pltpu.CompilerParams(
            collective_id=0, has_side_effects=True, vmem_limit_bytes=67000000
        ),
    )(x, gamma.reshape(1, D), w1, w2)
    return out[0]


def solution(mesh):
    return jax.shard_map(
        _block,
        mesh=mesh,
        in_specs=(P(("fsdp", "tp"), None), P(None), P("fsdp", "tp"), P("tp", "fsdp")),
        out_specs=P(("fsdp", "tp"), None),
        check_vma=False,
    )
```

```python
import functools

import jax
import jax.numpy as jnp
from jax import lax
from jax.experimental import pallas as pl
from jax.experimental.pallas import tpu as pltpu
from jax.sharding import PartitionSpec as P

EPS = 1e-6
MESH = pl.DeviceIdType.MESH
BF16, F32 = jnp.bfloat16, jnp.float32

D = 4096
FS = 3584
ROWS = 1024
NC = 7
CW = FS // NC
KB = D // 8
PR = 512
HR = PR // 2
LEAD2 = 512
HC = CW // 2
CUT1 = KB * 27 // 32
CUT2 = FS * 27 // 32


def _kernel(
    x_ref, gamma_ref, w1_ref, w2_ref,
    y_ref, xg, hg, w2g, d2d, sbuf, rs, sibp,
    w1v, xbuf, hbuf, wbuf, ubuf, dbuf, stage, tbuf, ybuf, sibv, rsv, xtv, obuf,
    w1_send, w1_recv, w2_send, w2_recv, x_send, x_recv,
    dd_send, dd_recv, rs_send, rs_recv, sp_send, sp_recv,
    l_sem, loc_sem, w_sem, o_sem,
):
    a, b = lax.axis_index("fsdp"), lax.axis_index("tp")
    z, yq = a // 2, a % 2
    c = b % 2
    to_zp = (lax.rem(z + 1, 4) * 2 + yq, b)
    to_zm = (lax.rem(z + 3, 4) * 2 + yq, b)
    to_yy = (z * 2 + 1 - yq, b)
    sib = (a, (b // 2) * 2 + 1 - c)
    par = (a, (1 - b // 2) * 2 + c)

    barrier = pltpu.get_barrier_semaphore()
    for dev in (to_zp, to_zm, to_yy, sib, par):
        pl.semaphore_signal(barrier, inc=1, device_id=dev, device_id_type=MESH)
    pl.semaphore_wait(barrier, 5)

    def remote(src, dst, ssem, rsem, dev):
        return pltpu.make_async_remote_copy(
            src_ref=src, dst_ref=dst, send_sem=ssem, recv_sem=rsem, device_id=dev, device_id_type=MESH
        )

    def messages(reg, own, send, recv, n, cut, lead):
        m = {}

        def blk(dz, dy):
            return (z + dz) * 2 + (1 - yq if dy else yq)

        def add(key, dev, dz, dy, lo, cnt, sent, got, first=False):
            i = len(m)
            dst = reg(blk(dz, dy), lo, cnt)
            m[key] = (remote(own(lo, cnt) if first else dst, dst, send(i), recv(i), dev), sent, got)

        always = None
        add("Y0", to_yy, 0, 0, 0, n, always, always, True)
        for d in (1, 2, 3):
            right = (z <= 2) & (z >= d - 1)
            left = (z >= 1) & (z <= 4 - d)
            skip = lead if d == 1 else 0
            if skip:
                add(("R", 0), to_zp, 0, 0, 0, skip, right, z >= 1, True)
                add(("L", 0), to_zm, 0, 0, 0, skip, left, z <= 2, True)
            add(("R", d), to_zp, 1 - d, 0, skip, n - skip, right, z >= d, d == 1)
            add(("L", d), to_zm, d - 1, 0, skip, n - skip, left, z <= 3 - d, d == 1)
            add(("YL", d), to_yy, -d, 0, 0, cut, z >= d, z >= d)
            add(("YR", d), to_yy, d, 0, 0, cut, z <= 3 - d, z <= 3 - d)
            add(("BR", d), to_zp, 1 - d, 1, cut, n - cut, right, z >= d)
            add(("BL", d), to_zm, d - 1, 1, cut, n - cut, left, z <= 3 - d)
        return m

    def when(cond, f):
        if cond is None:
            f()
        else:
            pl.when(cond)(f)

    def send(m, *keys):
        for k in keys:
            when(m[k][1], m[k][0].start)

    def got(m, *keys):
        for k in keys:
            when(m[k][2], m[k][0].wait_recv)

    def stage0(m):
        send(m, "Y0", ("R", 1), ("L", 1))

    def stage1(m):
        got(m, ("R", 1), ("L", 1))
        send(m, ("R", 2), ("L", 2), ("YL", 1), ("YR", 1))
        got(m, "Y0")
        send(m, ("BR", 1), ("BL", 1))

    def stage2(m):
        got(m, ("R", 2), ("L", 2))
        send(m, ("R", 3), ("L", 3), ("YL", 2), ("YR", 2))
        got(m, ("BR", 1), ("BL", 1))
        send(m, ("BR", 2), ("BL", 2))

    def stage3(m):
        got(m, ("R", 3), ("L", 3))
        send(m, ("YL", 3), ("YR", 3))
        got(m, ("BR", 2), ("BL", 2))
        send(m, ("BR", 3), ("BL", 3))

    def stage4(m):
        for d in (1, 2, 3):
            got(m, ("YL", d), ("YR", d))
        got(m, ("BR", 3), ("BL", 3))

    def w1_messages(j):
        def reg(s, lo, n):
            return w1v.at[j, pl.ds(pl.multiple_of(s * KB + lo, 16), n), :]

        def own(lo, n):
            return w1_ref.at[pl.ds(lo, n), pl.ds(j * CW, CW)]

        return messages(reg, own, lambda i: w1_send.at[j, i], lambda i: w1_recv.at[j, i], KB, CUT1, 0)

    w1m = [w1_messages(j) for j in range(NC)]
    loc = {}

    def s0(j):
        stage0(w1m[j])
        dst = w1v.at[j, pl.ds(pl.multiple_of(a * KB, KB), KB), :]
        cp = pltpu.make_async_copy(w1_ref.at[:, pl.ds(j * CW, CW)], dst, loc_sem.at[j])
        cp.start()
        loc[j] = cp

    def s1(j):
        stage1(w1m[j])

    def s2(j):
        stage2(w1m[j])

    def s3(j):
        stage3(w1m[j])

    def s4(j):
        stage4(w1m[j])
        loc[j].wait()

    w2m = messages(
        lambda s, lo, n: w2g.at[s, pl.ds(lo, n), :],
        lambda lo, n: w2_ref.at[pl.ds(lo, n), :],
        lambda i: w2_send.at[i], lambda i: w2_recv.at[i], FS, CUT2, LEAD2,
    )

    s0(0)
    s0(1)

    def x_in(r):
        return pltpu.make_async_copy(x_ref.at[pl.ds(r * HR, HR), :], xbuf.at[r % 2, pl.ds(0, HR), :], l_sem.at[r % 2])

    xs = {}
    x_in(0).start()
    for r in range(4):
        if r < 3:
            x_in(r + 1).start()
        x_in(r).wait()
        s = r % 2

        @pl.loop(0, HR // 32)
        def _(g):
            xf = xbuf[s, pl.ds(g * 32, 32), :].astype(F32)
            mu = jnp.mean(xf, axis=-1, keepdims=True)
            xc = xf - mu
            var = jnp.mean(jnp.square(xc), axis=-1, keepdims=True)
            xbuf[s, pl.ds(HR + g * 32, 32), :] = (xc * lax.rsqrt(var + EPS) * gamma_ref[...]).astype(BF16)

        mine = xg.at[pl.ds(r * HR, HR), :]
        cp = pltpu.make_async_copy(xbuf.at[s, pl.ds(HR, HR), :], mine, l_sem.at[2])
        cp.start()
        cp.wait()
        across = xg.at[pl.ds(pl.multiple_of(2 * ROWS + r * PR + c * HR, HR), HR), :]
        xs["p", r] = remote(mine, across, x_send.at[r], x_recv.at[r], par)
        xs["p", r].start()
        xs["s", r] = remote(mine, xg.at[pl.ds(ROWS + r * HR, HR), :], x_send.at[4 + r], x_recv.at[4 + r], sib)
        xs["s", r].start()

    def forward_x(r):
        xs["p", r].wait_recv()
        across = xg.at[pl.ds(pl.multiple_of(2 * ROWS + r * PR + c * HR, HR), HR), :]
        xs["f", r] = remote(across, across, x_send.at[8 + r], x_recv.at[8 + r], sib)
        xs["f", r].start()

    def h_tiles(n, p_of, j_of):
        def load(t, s):
            rows = pl.ds(pl.multiple_of(p_of(t) * PR, PR), PR)
            return pltpu.make_async_copy(xg.at[rows, :], xbuf.at[s], l_sem.at[s])

        def store(t, s):
            rows = pl.ds(pl.multiple_of(p_of(t) * PR, PR), PR)
            cols = pl.ds(pl.multiple_of(j_of(t) * CW, CW), CW)
            return pltpu.make_async_copy(hbuf.at[s], hg.at[rows, cols], l_sem.at[2 + s])

        load(0, 0).start()

        @pl.loop(0, n)
        def _(t):
            s = t % 2

            @pl.when(t + 1 < n)
            def _():
                load(t + 1, (t + 1) % 2).start()

            load(t, s).wait()

            @pl.when(t >= 2)
            def _():
                store(t, s).wait()

            j = j_of(t)

            @pl.loop(0, PR // HR)
            def _(r):
                rows = pl.ds(pl.multiple_of(r * HR, HR), HR)
                acc = jnp.dot(xbuf[s, rows, :], w1v[j], preferred_element_type=F32)
                hbuf[s, rows, :] = jax.nn.gelu(acc, approximate=True).astype(BF16)

            store(t, s).start()

        if n >= 2:
            store(n - 2, (n - 2) % 2).wait()
        store(n - 1, (n - 1) % 2).wait()

    def got_x(r):
        xs["f", r].wait_recv()

    for t in range(NC + 3):
        if 0 <= t - 2 < NC:
            s3(t - 2)
        if 0 <= t - 1 < NC:
            s2(t - 1)
        if t < NC:
            s1(t)
        if t + 2 < NC:
            s0(t + 2)
        if t == NC:
            send(w2m, ("R", 0), ("L", 0))
        if t == NC + 1:
            stage0(w2m)
        if t in (1, 2):
            forward_x(t - 1)
        if t < 3:
            continue
        j = t - 3
        s4(j)
        if j == 0:
            for r in range(4):
                xs["s", r].wait_recv()
            got_x(0)
        if j < 3:
            got_x(j + 1)
            h_tiles(
                6 + 2 * j,
                lambda n: jnp.minimum(n, 5 + j),
                lambda n: jnp.where(n < 5 + j, j, n - 5 - j),
            )
        elif j == 3:
            h_tiles(8, lambda n: n, lambda n: j)
        elif j < NC - 1:
            h_tiles(4, lambda n: 4 + n, lambda n: j)
        if j < 2:
            forward_x(j + 2)

    def h_load(p, s):
        rows = pl.ds(pl.multiple_of(p * PR, PR), PR)
        return pltpu.make_async_copy(hg.at[rows, :], xbuf.at[s, :, pl.ds(0, FS)], l_sem.at[s])

    def pick(kk, values):
        return sum(jnp.where(kk == k, v, 0) for k, v in enumerate(values) if v)

    def col_of(kk):
        i = pick(kk, (0, 1, 0, 2, 1, 3, 2, 3))
        dy = pick(kk, (0, 0, 1, 0, 1, 0, 1, 1))
        e = jnp.where(z < 2, z, 3 - z)
        v = jnp.where(i <= e, i - 1, i)
        v = jnp.where(z < 2, v, 3 - v)
        return jnp.where(i == 0, z, v) * 2 + lax.rem(yq + dy, 2)

    def dd_msg(n, s):
        return remote(ubuf.at[s, 1 - c], d2d.at[n], dd_send.at[s], dd_recv.at[n], sib)

    def rs_msg(n):
        return remote(sbuf.at[n], rs.at[n], rs_send.at[n], rs_recv.at[n], par)

    def sp_msg(n, s):
        return remote(tbuf.at[s], sibp.at[n], sp_send.at[s], sp_recv.at[n], sib)

    def d2d_in(n):
        return pltpu.make_async_copy(d2d.at[n], dbuf, l_sem.at[2])

    def sum_out(n):
        return pltpu.make_async_copy(stage, sbuf.at[n], l_sem.at[3])

    def pass_start(n, s):
        dd_msg(n, s).wait_recv()
        d2d_in(n).start()

    def pass_sum(n, s):
        d2d_in(n).wait()
        stage[...] = ubuf[s, c] + dbuf[...]
        sum_out(n).start()
        dd_msg(n, s).wait_send()

    def pass_send(n):
        sum_out(n).wait()
        rs_msg(n).start()

    def times_w2(s, w, out):
        @pl.loop(0, KB // HC)
        def _(r):
            cc = pl.ds(pl.multiple_of(r * HC, HC), HC)
            out(cc, jnp.dot(xbuf[s, :, pl.ds(0, FS)], wbuf[w, :, cc], preferred_element_type=F32))

    def w2_load(kk, w):
        @pl.when(kk == 0)
        def _():
            pltpu.make_async_copy(w2_ref, wbuf.at[w], w_sem.at[w]).start()

        @pl.when(kk > 0)
        def _():
            pltpu.make_async_copy(w2g.at[col_of(kk)], wbuf.at[w], w_sem.at[w]).start()

    def w2_wait(w):
        pltpu.make_async_copy(w2_ref, wbuf.at[w], w_sem.at[w]).wait()

    def partner_units(kk, w, first=False):
        if not first:
            h_load(4, 0).start()

        @pl.loop(0, 4)
        def _(q):
            s = q % 2
            n = kk * 4 + q
            if first:
                h_tiles(1, lambda t: 4 + q, lambda t: NC - 1)
                h_load(4 + q, s).start()
            else:

                @pl.when(q < 3)
                def _():
                    h_load(5 + q, 1 - s).start()

            if not first:

                @pl.when(q > 0)
                def _():
                    pass_start(n - 1, 1 - s)

            if first:

                @pl.when(q == 0)
                def _():
                    w2_wait(w)

            h_load(4 + q, s).wait()

            def out(cc, val):
                ubuf[s, 0, :, cc] = val[:HR]
                ubuf[s, 1, :, cc] = val[HR:]

            times_w2(s, w, out)
            dd_msg(n, s).start()

            if first:
                pass_start(n, s)
                pass_sum(n, s)
                pass_send(n)
            else:

                @pl.when(q > 0)
                def _():
                    pass_sum(n - 1, 1 - s)
                    pass_send(n - 1)

        if not first:
            n = kk * 4 + 3
            h_load(2, 0).start()
            h_load(3, 1).start()
            pass_start(n, 1)
            pass_sum(n, 1)
            pass_send(n)

    def sibling_units(kk, w):
        @pl.loop(0, 2)
        def _(p):
            h_load(2 + p, p).wait()

            @pl.when(kk > 0)
            def _():
                sp_msg(kk * 2 + p - 2, p).wait_send()

            def out(cc, val):
                tbuf[p, :, cc] = val

            times_w2(p, w, out)
            sp_msg(kk * 2 + p, p).start()

    def finish(kk, w):
        for p in range(2):
            h_load(p, p).start()
        cols = pl.ds(pl.multiple_of(col_of(kk) * KB, KB), KB)

        @pl.loop(0, 2)
        def _(p):
            rows = pl.ds(pl.multiple_of(p * PR, PR), PR)
            n = kk * 2 + p
            cx = pltpu.make_async_copy(x_ref.at[rows, cols], xtv, l_sem.at[2])
            cx.start()
            sp_msg(n, p).wait_recv()
            cs = pltpu.make_async_copy(sibp.at[n], sibv, l_sem.at[3])
            cs.start()
            h_load(p, p).wait()

            def out(cc, val):
                ybuf[:, cc] = val

            times_w2(p, w, out)
            cs.wait()
            cx.wait()
            for r in range(2):
                rs_msg(kk * 4 + p * 2 + r).wait_recv()
                pltpu.make_async_copy(rs.at[kk * 4 + p * 2 + r], rsv.at[r], l_sem.at[2 + r]).start()

            co = pltpu.make_async_copy(obuf, y_ref.at[rows, cols], o_sem)
            for r in range(2):
                rr = pl.ds(r * HR, HR)
                pltpu.make_async_copy(rs.at[kk * 4 + p * 2 + r], rsv.at[r], l_sem.at[2 + r]).wait()
                if r == 0:

                    @pl.when(n > 0)
                    def _():
                        co.wait()

                total = ybuf[rr, :] + sibv[rr, :] + rsv[r]
                obuf[rr, :] = (xtv[rr, :].astype(F32) + total).astype(BF16)
            co.start()

    w2_load(0, 0)
    partner_units(0, 0, True)
    h_tiles(2, lambda n: 2 + n, lambda n: 4)

    @pl.loop(1, 11)
    def _(kk):
        w = kk % 4

        @pl.when(kk == 1)
        def _():
            got(w2m, ("R", 0), ("L", 0), ("R", 1), ("L", 1))
            send(w2m, ("R", 2), ("L", 2), ("YL", 1), ("YR", 1))

        @pl.when(kk == 2)
        def _():
            got(w2m, "Y0")
            send(w2m, ("BR", 1), ("BL", 1))

        @pl.when(kk == 3)
        def _():
            stage2(w2m)

        @pl.when(kk == 4)
        def _():
            got(w2m, ("YL", 1), ("YR", 1))

        @pl.when(kk == 5)
        def _():
            stage3(w2m)

        @pl.when(kk == 6)
        def _():
            got(w2m, ("YL", 2), ("YR", 2))

        @pl.when(kk == 7)
        def _():
            got(w2m, ("YL", 3), ("YR", 3), ("BR", 3), ("BL", 3))

        @pl.when(kk < 8)
        def _():
            w2_load(kk, w)
            w2_wait(w)
            partner_units(kk, w)

        @pl.when(kk == 2)
        def _():
            h_load(2, 0).wait()
            h_load(3, 1).wait()
            h_tiles(10, lambda n: n % 4, lambda n: 6 - n // 4)
            h_load(2, 0).start()
            h_load(3, 1).start()
            sibling_units(0, 0)
            h_load(2, 0).start()
            h_load(3, 1).start()

        @pl.when(kk == 8)
        def _():
            h_load(2, 0).start()
            h_load(3, 1).start()

        @pl.when((kk > 1) & (kk < 9))
        def _():
            sibling_units(kk - 1, (kk + 3) % 4)

        @pl.when(kk == 1)
        def _():
            h_load(2, 0).wait()
            h_load(3, 1).wait()

        @pl.when(kk > 2)
        def _():
            finish(kk - 3, (kk + 1) % 4)

    pltpu.make_async_copy(obuf, y_ref.at[pl.ds(0, PR), pl.ds(0, KB)], o_sem).wait()
    for p in range(2):
        sp_msg(14 + p, p).wait_send()

    for m in (*w1m, w2m):
        for cp, sent, _ in m.values():
            when(sent, cp.wait_send)
    for cp in xs.values():
        cp.wait_send()

    @pl.loop(0, 32)
    def _(n):
        rs_msg(n).wait_send()


def _block(x, gamma, w1, w2):
    hbm = pl.BlockSpec(memory_space=pl.ANY)
    out = pl.pallas_call(
        _kernel,
        name="mlp",
        out_shape=[
            jax.ShapeDtypeStruct((ROWS, D), BF16),
            jax.ShapeDtypeStruct((4 * ROWS, D), BF16),
            jax.ShapeDtypeStruct((4 * ROWS, FS), BF16),
            jax.ShapeDtypeStruct((8, FS, KB), BF16),
            jax.ShapeDtypeStruct((32, HR, KB), F32),
            jax.ShapeDtypeStruct((32, HR, KB), F32),
            jax.ShapeDtypeStruct((32, HR, KB), F32),
            jax.ShapeDtypeStruct((16, PR, KB), F32),
        ],
        in_specs=[hbm, pl.BlockSpec(memory_space=pltpu.VMEM), hbm, hbm],
        out_specs=[hbm] * 8,
        scratch_shapes=[
            pltpu.VMEM((NC, D, CW), BF16),
            pltpu.VMEM((2, PR, D), BF16),
            pltpu.VMEM((2, PR, CW), BF16),
            pltpu.VMEM((4, FS, KB), BF16),
            pltpu.VMEM((2, 2, HR, KB), F32),
            pltpu.VMEM((HR, KB), F32),
            pltpu.VMEM((HR, KB), F32),
            pltpu.VMEM((2, PR, KB), F32),
            pltpu.VMEM((PR, KB), F32),
            pltpu.VMEM((PR, KB), F32),
            pltpu.VMEM((2, HR, KB), F32),
            pltpu.VMEM((PR, KB), BF16),
            pltpu.VMEM((PR, KB), BF16),
            pltpu.SemaphoreType.DMA((NC, 19)),
            pltpu.SemaphoreType.DMA((NC, 19)),
            pltpu.SemaphoreType.DMA((21,)),
            pltpu.SemaphoreType.DMA((21,)),
            pltpu.SemaphoreType.DMA((12,)),
            pltpu.SemaphoreType.DMA((12,)),
            pltpu.SemaphoreType.DMA((2,)),
            pltpu.SemaphoreType.DMA((32,)),
            pltpu.SemaphoreType.DMA((32,)),
            pltpu.SemaphoreType.DMA((32,)),
            pltpu.SemaphoreType.DMA((2,)),
            pltpu.SemaphoreType.DMA((16,)),
            pltpu.SemaphoreType.DMA((4,)),
            pltpu.SemaphoreType.DMA((NC,)),
            pltpu.SemaphoreType.DMA((4,)),
            pltpu.SemaphoreType.DMA,
        ],
        compiler_params=pltpu.CompilerParams(
            collective_id=0, has_side_effects=True, vmem_limit_bytes=67000000
        ),
    )(x, gamma.reshape(1, D), w1, w2)
    return out[0]


def solution(mesh):
    return jax.shard_map(
        _block,
        mesh=mesh,
        in_specs=(P(("fsdp", "tp"), None), P(None), P("fsdp", "tp"), P("tp", "fsdp")),
        out_specs=P(("fsdp", "tp"), None),
        check_vma=False,
    )
```

```python
import functools

import jax
import jax.numpy as jnp
from jax import lax
from jax.experimental import pallas as pl
from jax.experimental.pallas import tpu as pltpu
from jax.sharding import PartitionSpec as P

EPS = 1e-6
MESH = pl.DeviceIdType.MESH
BF16, F32 = jnp.bfloat16, jnp.float32

D = 4096
FS = 3584
ROWS = 1024
NC = 7
CW = FS // NC
KB = D // 8
PR = 512
HR = PR // 2
LEAD2 = 512
HC = CW // 2
CUT1 = KB * 27 // 32
CUT2 = FS * 27 // 32


def _kernel(
    x_ref, gamma_ref, w1_ref, w2_ref,
    y_ref, xg, hg, w2g, d2d, sbuf, rs, sibp,
    w1v, xbuf, hbuf, wbuf, ubuf, dbuf, stage, tbuf, ybuf, sibv, rsv, xtv, obuf,
    w1_send, w1_recv, w2_send, w2_recv, x_send, x_recv,
    dd_send, dd_recv, rs_send, rs_recv, sp_send, sp_recv,
    l_sem, loc_sem, w_sem, o_sem,
):
    a, b = lax.axis_index("fsdp"), lax.axis_index("tp")
    z, yq = a // 2, a % 2
    c = b % 2
    to_zp = (lax.rem(z + 1, 4) * 2 + yq, b)
    to_zm = (lax.rem(z + 3, 4) * 2 + yq, b)
    to_yy = (z * 2 + 1 - yq, b)
    sib = (a, (b // 2) * 2 + 1 - c)
    par = (a, (1 - b // 2) * 2 + c)

    barrier = pltpu.get_barrier_semaphore()
    for dev in (to_zp, to_zm, to_yy, sib, par):
        pl.semaphore_signal(barrier, inc=1, device_id=dev, device_id_type=MESH)
    pl.semaphore_wait(barrier, 5)

    def remote(src, dst, ssem, rsem, dev):
        return pltpu.make_async_remote_copy(
            src_ref=src, dst_ref=dst, send_sem=ssem, recv_sem=rsem, device_id=dev, device_id_type=MESH
        )

    def messages(reg, own, send, recv, n, cut, lead):
        m = {}

        def blk(dz, dy):
            return (z + dz) * 2 + (1 - yq if dy else yq)

        def add(key, dev, dz, dy, lo, cnt, sent, got, first=False, part=None):
            i = len(m)
            dst = reg(blk(dz, dy), lo, cnt, part)
            m[key] = (remote(own(lo, cnt, part) if first else dst, dst, send(i), recv(i), dev), sent, got)

        always = None
        if lead:
            add("Y0", to_yy, 0, 0, 0, n, always, always, True, 0)
            add("Y1", to_yy, 0, 0, 0, n, always, always, True, 1)
            add(("R", 0), to_zp, 0, 0, 0, lead, z <= 2, z >= 1, True)
            add(("L", 0), to_zm, 0, 0, 0, lead, z >= 1, z <= 2, True)
        else:
            add("Y0", to_yy, 0, 0, 0, n, always, always, True)
        for d in (1, 2, 3):
            right = (z <= 2) & (z >= d - 1)
            left = (z >= 1) & (z <= 4 - d)
            skip = lead if d == 1 else 0
            for part in (0, 1) if lead and d < 3 else (None,):
                k = (d,) if part is None else (d, part)
                add(("R", *k), to_zp, 1 - d, 0, skip, n - skip, right, z >= d, d == 1, part)
                add(("L", *k), to_zm, d - 1, 0, skip, n - skip, left, z <= 3 - d, d == 1, part)
            add(("YL", d), to_yy, -d, 0, 0, cut, z >= d, z >= d)
            add(("YR", d), to_yy, d, 0, 0, cut, z <= 3 - d, z <= 3 - d)
            add(("BR", d), to_zp, 1 - d, 1, cut, n - cut, right, z >= d)
            add(("BL", d), to_zm, d - 1, 1, cut, n - cut, left, z <= 3 - d)
        return m

    def when(cond, f):
        if cond is None:
            f()
        else:
            pl.when(cond)(f)

    def send(m, *keys):
        for k in keys:
            when(m[k][1], m[k][0].start)

    def got(m, *keys):
        for k in keys:
            when(m[k][2], m[k][0].wait_recv)

    def stage0(m):
        send(m, "Y0", ("R", 1), ("L", 1))

    def stage1(m):
        got(m, ("R", 1), ("L", 1))
        send(m, ("R", 2), ("L", 2), ("YL", 1), ("YR", 1))
        got(m, "Y0")
        send(m, ("BR", 1), ("BL", 1))

    def stage2(m):
        got(m, ("R", 2), ("L", 2))
        send(m, ("R", 3), ("L", 3), ("YL", 2), ("YR", 2))
        got(m, ("BR", 1), ("BL", 1))
        send(m, ("BR", 2), ("BL", 2))

    def stage3(m):
        got(m, ("R", 3), ("L", 3))
        send(m, ("YL", 3), ("YR", 3))
        got(m, ("BR", 2), ("BL", 2))
        send(m, ("BR", 3), ("BL", 3))

    def stage4(m):
        for d in (1, 2, 3):
            got(m, ("YL", d), ("YR", d))
        got(m, ("BR", 3), ("BL", 3))

    def w1_messages(j):
        def reg(s, lo, n, part):
            return w1v.at[j, pl.ds(pl.multiple_of(s * KB + lo, 16), n), :]

        def own(lo, n, part):
            return w1_ref.at[pl.ds(lo, n), pl.ds(j * CW, CW)]

        return messages(reg, own, lambda i: w1_send.at[j, i], lambda i: w1_recv.at[j, i], KB, CUT1, 0)

    w1m = [w1_messages(j) for j in range(NC)]
    loc = {}

    def s0(j):
        stage0(w1m[j])
        dst = w1v.at[j, pl.ds(pl.multiple_of(a * KB, KB), KB), :]
        cp = pltpu.make_async_copy(w1_ref.at[:, pl.ds(j * CW, CW)], dst, loc_sem.at[j])
        cp.start()
        loc[j] = cp

    def s1(j):
        stage1(w1m[j])

    def s2(j):
        stage2(w1m[j])

    def s3(j):
        stage3(w1m[j])

    def s4(j):
        stage4(w1m[j])
        loc[j].wait()

    def half(part):
        return slice(None) if part is None else pl.ds(part * HC, HC)

    w2m = messages(
        lambda s, lo, n, part: w2g.at[s, pl.ds(lo, n), half(part)],
        lambda lo, n, part: w2_ref.at[pl.ds(lo, n), half(part)],
        lambda i: w2_send.at[i], lambda i: w2_recv.at[i], FS, CUT2, LEAD2,
    )

    s0(0)
    s0(1)

    def x_in(r):
        return pltpu.make_async_copy(x_ref.at[pl.ds(r * HR, HR), :], xbuf.at[r % 2, pl.ds(0, HR), :], l_sem.at[r % 2])

    xs = {}
    x_in(0).start()
    for r in range(4):
        if r < 3:
            x_in(r + 1).start()
        x_in(r).wait()
        s = r % 2

        @pl.loop(0, HR // 32)
        def _(g):
            xf = xbuf[s, pl.ds(g * 32, 32), :].astype(F32)
            mu = jnp.mean(xf, axis=-1, keepdims=True)
            xc = xf - mu
            var = jnp.mean(jnp.square(xc), axis=-1, keepdims=True)
            xbuf[s, pl.ds(HR + g * 32, 32), :] = (xc * lax.rsqrt(var + EPS) * gamma_ref[...]).astype(BF16)

        mine = xg.at[pl.ds(r * HR, HR), :]
        cp = pltpu.make_async_copy(xbuf.at[s, pl.ds(HR, HR), :], mine, l_sem.at[2])
        cp.start()
        cp.wait()
        across = xg.at[pl.ds(pl.multiple_of(2 * ROWS + r * PR + c * HR, HR), HR), :]
        xs["p", r] = remote(mine, across, x_send.at[r], x_recv.at[r], par)
        xs["p", r].start()
        xs["s", r] = remote(mine, xg.at[pl.ds(ROWS + r * HR, HR), :], x_send.at[4 + r], x_recv.at[4 + r], sib)
        xs["s", r].start()

    def forward_x(r):
        xs["p", r].wait_recv()
        across = xg.at[pl.ds(pl.multiple_of(2 * ROWS + r * PR + c * HR, HR), HR), :]
        xs["f", r] = remote(across, across, x_send.at[8 + r], x_recv.at[8 + r], sib)
        xs["f", r].start()

    def h_tiles(n, p_of, j_of):
        def load(t, s):
            rows = pl.ds(pl.multiple_of(p_of(t) * PR, PR), PR)
            return pltpu.make_async_copy(xg.at[rows, :], xbuf.at[s], l_sem.at[s])

        def store(t, s):
            rows = pl.ds(pl.multiple_of(p_of(t) * PR, PR), PR)
            cols = pl.ds(pl.multiple_of(j_of(t) * CW, CW), CW)
            return pltpu.make_async_copy(hbuf.at[s], hg.at[rows, cols], l_sem.at[2 + s])

        load(0, 0).start()

        @pl.loop(0, n)
        def _(t):
            s = t % 2

            @pl.when(t + 1 < n)
            def _():
                load(t + 1, (t + 1) % 2).start()

            load(t, s).wait()

            @pl.when(t >= 2)
            def _():
                store(t, s).wait()

            j = j_of(t)

            @pl.loop(0, PR // HR)
            def _(r):
                rows = pl.ds(pl.multiple_of(r * HR, HR), HR)
                acc = jnp.dot(xbuf[s, rows, :], w1v[j], preferred_element_type=F32)
                hbuf[s, rows, :] = jax.nn.gelu(acc, approximate=True).astype(BF16)

            store(t, s).start()

        if n >= 2:
            store(n - 2, (n - 2) % 2).wait()
        store(n - 1, (n - 1) % 2).wait()

    def got_x(r):
        xs["f", r].wait_recv()

    for t in range(NC + 3):
        if 0 <= t - 2 < NC:
            s3(t - 2)
        if 0 <= t - 1 < NC:
            s2(t - 1)
        if t < NC:
            s1(t)
        if t + 2 < NC:
            s0(t + 2)
        if t == NC:
            send(w2m, ("R", 0), ("L", 0))
        if t == NC + 1:
            send(w2m, ("R", 1, 0), ("L", 1, 0), "Y0", ("R", 1, 1), ("L", 1, 1), "Y1")
        if t in (1, 2):
            forward_x(t - 1)
        if t < 3:
            continue
        j = t - 3
        s4(j)
        if j == 0:
            for r in range(4):
                xs["s", r].wait_recv()
            got_x(0)
        if j < 3:
            got_x(j + 1)
            h_tiles(
                6 + 2 * j,
                lambda n: jnp.minimum(n, 5 + j),
                lambda n: jnp.where(n < 5 + j, j, n - 5 - j),
            )
        elif j == 3:
            h_tiles(8, lambda n: n, lambda n: j)
        elif j < NC - 1:
            h_tiles(4, lambda n: 4 + n, lambda n: j)
        if j < 2:
            forward_x(j + 2)

    def h_load(p, s):
        rows = pl.ds(pl.multiple_of(p * PR, PR), PR)
        return pltpu.make_async_copy(hg.at[rows, :], xbuf.at[s, :, pl.ds(0, FS)], l_sem.at[s])

    def pick(kk, values):
        return sum(jnp.where(kk == k, v, 0) for k, v in enumerate(values) if v)

    def col_of(kk):
        i = pick(kk, (0, 1, 0, 1, 2, 2, 3, 3))
        dy = pick(kk, (0, 0, 1, 1, 0, 1, 0, 1))
        e = jnp.where(z < 2, z, 3 - z)
        v = jnp.where(i <= e, i - 1, i)
        v = jnp.where(z < 2, v, 3 - v)
        v = jnp.where(z == 2, pick(i, (0, 1, 3, 0)), v)
        return jnp.where(i == 0, z, v) * 2 + lax.rem(yq + dy, 2)

    def source(kk, h):
        mixed = (kk == 1) | (kk == 2)
        return col_of(jnp.where(mixed, 1 + h, kk)), pl.multiple_of(jnp.where(mixed, kk - 1, h) * HC, HC)

    def dd_msg(n, s):
        return remote(ubuf.at[s, 1 - c], d2d.at[n], dd_send.at[s], dd_recv.at[n], sib)

    def rs_msg(n):
        return remote(sbuf.at[n], rs.at[n], rs_send.at[n], rs_recv.at[n], par)

    def sp_msg(n, s):
        return remote(tbuf.at[s], sibp.at[n], sp_send.at[s], sp_recv.at[n], sib)

    def d2d_in(n):
        return pltpu.make_async_copy(d2d.at[n], dbuf, l_sem.at[2])

    def sum_out(n):
        return pltpu.make_async_copy(stage, sbuf.at[n], l_sem.at[3])

    def pass_start(n, s):
        dd_msg(n, s).wait_recv()
        d2d_in(n).start()

    def pass_sum(n, s):
        d2d_in(n).wait()
        stage[...] = ubuf[s, c] + dbuf[...]
        sum_out(n).start()
        dd_msg(n, s).wait_send()

    def pass_send(n):
        sum_out(n).wait()
        rs_msg(n).start()

    def times_w2(s, w, out):
        @pl.loop(0, KB // HC)
        def _(r):
            cc = pl.ds(pl.multiple_of(r * HC, HC), HC)
            out(cc, jnp.dot(xbuf[s, :, pl.ds(0, FS)], wbuf[w, :, cc], preferred_element_type=F32))

    def w2_load(kk, w):
        @pl.when(kk == 0)
        def _():
            pltpu.make_async_copy(w2_ref, wbuf.at[w], w_sem.at[w]).start()

        @pl.when(kk > 0)
        def _():
            for h in range(2):
                shard, off = source(kk, h)
                src = w2g.at[shard, :, pl.ds(off, HC)]
                pltpu.make_async_copy(src, wbuf.at[w, :, pl.ds(h * HC, HC)], w_sem.at[w]).start()

    def w2_wait(w):
        pltpu.make_async_copy(w2_ref, wbuf.at[w], w_sem.at[w]).wait()

    def partner_units(kk, w, first=False):
        if not first:
            h_load(4, 0).start()

        @pl.loop(0, 4)
        def _(q):
            s = q % 2
            n = kk * 4 + q
            if first:
                h_tiles(1, lambda t: 4 + q, lambda t: NC - 1)
                h_load(4 + q, s).start()
            else:

                @pl.when(q < 3)
                def _():
                    h_load(5 + q, 1 - s).start()

            if not first:

                @pl.when(q > 0)
                def _():
                    pass_start(n - 1, 1 - s)

            if first:

                @pl.when(q == 0)
                def _():
                    w2_wait(w)

            h_load(4 + q, s).wait()

            def out(cc, val):
                ubuf[s, 0, :, cc] = val[:HR]
                ubuf[s, 1, :, cc] = val[HR:]

            times_w2(s, w, out)
            dd_msg(n, s).start()

            if first:
                pass_start(n, s)
                pass_sum(n, s)
                pass_send(n)
            else:

                @pl.when(q > 0)
                def _():
                    pass_sum(n - 1, 1 - s)
                    pass_send(n - 1)

        if not first:
            n = kk * 4 + 3
            h_load(2, 0).start()
            h_load(3, 1).start()
            pass_start(n, 1)
            pass_sum(n, 1)
            pass_send(n)

    def sibling_units(kk, w):
        @pl.loop(0, 2)
        def _(p):
            h_load(2 + p, p).wait()

            @pl.when(kk > 0)
            def _():
                sp_msg(kk * 2 + p - 2, p).wait_send()

            def out(cc, val):
                tbuf[p, :, cc] = val

            times_w2(p, w, out)
            sp_msg(kk * 2 + p, p).start()

    def finish(kk, w):
        for p in range(2):
            h_load(p, p).start()
        cols = []
        for h in range(2):
            shard, off = source(kk, h)
            cols.append(pl.ds(pl.multiple_of(shard * KB + off, HC), HC))

        @pl.loop(0, 2)
        def _(p):
            rows = pl.ds(pl.multiple_of(p * PR, PR), PR)
            n = kk * 2 + p
            cx = [pltpu.make_async_copy(x_ref.at[rows, cols[h]], xtv.at[:, half(h)], l_sem.at[2]) for h in range(2)]
            for cp in cx:
                cp.start()
            sp_msg(n, p).wait_recv()
            cs = pltpu.make_async_copy(sibp.at[n], sibv, l_sem.at[3])
            cs.start()
            h_load(p, p).wait()

            def out(cc, val):
                ybuf[:, cc] = val

            times_w2(p, w, out)
            cs.wait()
            pltpu.make_async_copy(x_ref.at[rows, pl.ds(0, KB)], xtv, l_sem.at[2]).wait()
            for r in range(2):
                rs_msg(kk * 4 + p * 2 + r).wait_recv()
                pltpu.make_async_copy(rs.at[kk * 4 + p * 2 + r], rsv.at[r], l_sem.at[2 + r]).start()

            co = [pltpu.make_async_copy(obuf.at[:, half(h)], y_ref.at[rows, cols[h]], o_sem) for h in range(2)]
            for r in range(2):
                rr = pl.ds(r * HR, HR)
                pltpu.make_async_copy(rs.at[kk * 4 + p * 2 + r], rsv.at[r], l_sem.at[2 + r]).wait()
                if r == 0:

                    @pl.when(n > 0)
                    def _():
                        pltpu.make_async_copy(obuf, y_ref.at[rows, pl.ds(0, KB)], o_sem).wait()

                total = ybuf[rr, :] + sibv[rr, :] + rsv[r]
                obuf[rr, :] = (xtv[rr, :].astype(F32) + total).astype(BF16)
            for cp in co:
                cp.start()

    w2_load(0, 0)
    partner_units(0, 0, True)

    inner = (z == 1) | (z == 2)

    @pl.loop(1, 10)
    def _(kk):
        w = kk % 4

        @pl.when(kk == 1)
        def _():
            got(w2m, ("R", 0), ("L", 0), ("R", 1, 0), ("L", 1, 0), "Y0")
            send(w2m, ("R", 2, 0), ("L", 2, 0))

        @pl.when(kk == 2)
        def _():
            got(w2m, ("R", 1, 1), ("L", 1, 1), "Y1")
            send(w2m, ("YL", 1), ("YR", 1), ("BR", 1), ("BL", 1), ("R", 2, 1), ("L", 2, 1))

        @pl.when(kk == 3)
        def _():
            pl.when(z == 0)(w2m["YR", 1][0].wait_recv)
            pl.when(z > 0)(w2m["YL", 1][0].wait_recv)
            got(w2m, ("BR", 1), ("BL", 1))

        @pl.when(kk == 5)
        def _():
            pl.when(z == 0)(w2m["YR", 2][0].wait_recv)
            pl.when(z == 3)(w2m["YL", 2][0].wait_recv)
            pl.when(inner)(w2m["YR", 1][0].wait_recv)
            got(w2m, ("BR", 2), ("BL", 2))

        @pl.when(kk == 7)
        def _():
            finish(4, 0)
            pl.when(z == 1)(w2m["YR", 2][0].wait_recv)
            pl.when(z == 2)(w2m["YL", 2][0].wait_recv)
            got(w2m, ("YL", 3), ("YR", 3), ("BR", 3), ("BL", 3))

        @pl.when(kk < 8)
        def _():
            w2_load(kk, w)
            w2_wait(w)
            partner_units(kk, w)

        @pl.when(kk == 3)
        def _():
            got(w2m, ("R", 2, 0), ("L", 2, 0), ("R", 2, 1), ("L", 2, 1))
            send(w2m, ("BR", 2), ("BL", 2), ("R", 3), ("L", 3), ("YL", 2), ("YR", 2))

        @pl.when(kk == 5)
        def _():
            got(w2m, ("R", 3), ("L", 3))
            send(w2m, ("BR", 3), ("BL", 3), ("YL", 3), ("YR", 3))

        @pl.when(kk == 2)
        def _():
            h_load(2, 0).wait()
            h_load(3, 1).wait()
            h_tiles(12, lambda n: n % 4, lambda n: 4 + n // 4)
            h_load(2, 0).start()
            h_load(3, 1).start()
            sibling_units(0, 0)
            h_load(2, 0).start()
            h_load(3, 1).start()

        @pl.when(kk == 8)
        def _():
            h_load(2, 0).start()
            h_load(3, 1).start()

        @pl.when((kk > 1) & (kk < 9))
        def _():
            sibling_units(kk - 1, (kk + 3) % 4)

        @pl.when(kk == 1)
        def _():
            h_load(2, 0).wait()
            h_load(3, 1).wait()

        @pl.when(kk > 2)
        def _():
            n = jnp.where(kk < 7, kk - 3, kk - 2)
            finish(n, n % 4)

    pltpu.make_async_copy(obuf, y_ref.at[pl.ds(0, PR), pl.ds(0, KB)], o_sem).wait()
    for p in range(2):
        sp_msg(14 + p, p).wait_send()

    for m in (*w1m, w2m):
        for cp, sent, _ in m.values():
            when(sent, cp.wait_send)
    for cp in xs.values():
        cp.wait_send()

    @pl.loop(0, 32)
    def _(n):
        rs_msg(n).wait_send()


def _block(x, gamma, w1, w2):
    hbm = pl.BlockSpec(memory_space=pl.ANY)
    out = pl.pallas_call(
        _kernel,
        name="mlp",
        out_shape=[
            jax.ShapeDtypeStruct((ROWS, D), BF16),
            jax.ShapeDtypeStruct((4 * ROWS, D), BF16),
            jax.ShapeDtypeStruct((4 * ROWS, FS), BF16),
            jax.ShapeDtypeStruct((8, FS, KB), BF16),
            jax.ShapeDtypeStruct((32, HR, KB), F32),
            jax.ShapeDtypeStruct((32, HR, KB), F32),
            jax.ShapeDtypeStruct((32, HR, KB), F32),
            jax.ShapeDtypeStruct((16, PR, KB), F32),
        ],
        in_specs=[hbm, pl.BlockSpec(memory_space=pltpu.VMEM), hbm, hbm],
        out_specs=[hbm] * 8,
        scratch_shapes=[
            pltpu.VMEM((NC, D, CW), BF16),
            pltpu.VMEM((2, PR, D), BF16),
            pltpu.VMEM((2, PR, CW), BF16),
            pltpu.VMEM((4, FS, KB), BF16),
            pltpu.VMEM((2, 2, HR, KB), F32),
            pltpu.VMEM((HR, KB), F32),
            pltpu.VMEM((HR, KB), F32),
            pltpu.VMEM((2, PR, KB), F32),
            pltpu.VMEM((PR, KB), F32),
            pltpu.VMEM((PR, KB), F32),
            pltpu.VMEM((2, HR, KB), F32),
            pltpu.VMEM((PR, KB), BF16),
            pltpu.VMEM((PR, KB), BF16),
            pltpu.SemaphoreType.DMA((NC, 19)),
            pltpu.SemaphoreType.DMA((NC, 19)),
            pltpu.SemaphoreType.DMA((26,)),
            pltpu.SemaphoreType.DMA((26,)),
            pltpu.SemaphoreType.DMA((12,)),
            pltpu.SemaphoreType.DMA((12,)),
            pltpu.SemaphoreType.DMA((2,)),
            pltpu.SemaphoreType.DMA((32,)),
            pltpu.SemaphoreType.DMA((32,)),
            pltpu.SemaphoreType.DMA((32,)),
            pltpu.SemaphoreType.DMA((2,)),
            pltpu.SemaphoreType.DMA((16,)),
            pltpu.SemaphoreType.DMA((4,)),
            pltpu.SemaphoreType.DMA((NC,)),
            pltpu.SemaphoreType.DMA((4,)),
            pltpu.SemaphoreType.DMA,
        ],
        compiler_params=pltpu.CompilerParams(
            collective_id=0, has_side_effects=True, vmem_limit_bytes=67000000
        ),
    )(x, gamma.reshape(1, D), w1, w2)
    return out[0]


def solution(mesh):
    return jax.shard_map(
        _block,
        mesh=mesh,
        in_specs=(P(("fsdp", "tp"), None), P(None), P("fsdp", "tp"), P("tp", "fsdp")),
        out_specs=P(("fsdp", "tp"), None),
        check_vma=False,
    )
```
